512 devices in a mesh: band: 16 (over x, z_hi), fft: 32 (over y, z_lo, core).
Axes of the slice: x: 4, y: 8, z: 8 (z_hi: 4, z_lo: 2; z = z_hi * 2 + z_lo), core: 2. Of those that a mesh axis runs over, the one named last changes fastest.
Arguments:
- wave: float32 [2, 32, 128, 128, 128], P(None, 'band', 'fft'), may hold values from -6 to 6
- previous: float32 [2, 32, 128, 128, 128], P(None, 'band', 'fft'), may hold values from -6 to 6
- potential: float32 [128, 128, 128], P('band', 'fft'), may hold values from -1.5 to 1.5
- column_extent: int32 [128, 128], P('fft'), may hold values from -1 to 31, as said below
- metric: float32 [3], replicated, may hold values from 0.5 to 2
- center: float32 [1], replicated, may hold values from 0.5 to 2
- halfwidth: float32 [1], replicated, may hold values from 1 to 3
Outputs:
- filtered: float32 [2, 32, 128, 128, 128], P(None, 'band', 'fft')
The draws below stay inside these ranges and needn't reach their ends.
Inputs may be any that keep to these rules, and one draw needn't show every extreme that they name: `column_extent`: every entry is -1 where |s(gx)| >= 32 or |s(gy)| >= 32, with s the signed index of the steps. Some column reaches the maximum.
All inputs are finite; a program needn't handle non-finite values.
Results may differ from the reference program's by a relative error of at most 0.00005.
Values sent between devices are 32-bit elements; how exact they have to be, the bound alone decides.
No kernel may reach another device: no remote copies, remote signals or barrier semaphores. Data moves between devices by JAX's collectives and lax.ppermute only.
A program may use at most 64 MiB of HBM per device.

```python
import math
import jax
import jax.numpy as jnp
from jax import lax

NX = 128
NY = 128
NZ = 128
BANDS = 32


def draw_column_extent(key, part):
    first_key, second_key = jax.random.split(key, 2)
    weights = jax.random.randint(first_key, (3,), 1, 5).astype(jnp.int32)
    largest = NZ // 4 - 1
    base_room = weights[2] * largest * largest
    radius_sq = base_room + jax.random.randint(second_key, (), 0, 1024).astype(jnp.int32) * (base_room // 1024 + 1)
    index_x = jnp.arange(NX, dtype=jnp.int32)
    index_y = jnp.arange(NY, dtype=jnp.int32)
    signed_x = jnp.where(index_x < NX // 2, index_x, index_x - NX)
    signed_y = jnp.where(index_y < NY // 2, index_y, index_y - NY)
    room_left = radius_sq - weights[0] * signed_x[:, None] ** 2 - weights[1] * signed_y[None, :] ** 2
    heights = jnp.arange(largest + 1, dtype=jnp.int32)
    counted = jnp.sum((weights[2] * heights[None, None, :] ** 2 <= room_left[:, :, None]).astype(jnp.int32), axis=2) - 1
    in_box = (jnp.abs(signed_x)[:, None] < NX // 4) & (jnp.abs(signed_y)[None, :] < NY // 4)
    return jnp.where(in_box, counted, -1).astype(jnp.int32)


def shard_levels(key, dims, shards, smallest, high):
    factor_of, own = 1.0, jax.random.fold_in(key, 6)
    for dim, blocks in shards:
        steps = jnp.exp(jax.random.uniform(jax.random.fold_in(own, dim), (blocks,), jnp.float32, smallest / len(shards), high / len(shards)))
        factor_of = factor_of * jnp.repeat(steps, dims[dim] // blocks).reshape([-1 if axis == dim else 1 for axis in range(len(dims))])
    return factor_of


def noise(rng, extent, deviation, bound, cuts=(), kind=jnp.bfloat16):
    values = jax.random.normal(rng, extent, jnp.float32) * deviation
    if len(cuts) > 0:
        values = shard_levels(rng, extent, cuts, -0.22, 0.18) * values
    return jnp.clip(values, min=-bound, max=bound).astype(kind)


def setup_inputs(seed: int = 0) -> dict:
    keys = jax.random.split(jax.random.key(seed), 8)
    return {
        "wave": noise(keys[0], (2, BANDS, NX, NZ, NY), 1.0, 6.0, ((1, 16), (2, 32)), jnp.float32),
        "previous": noise(keys[1], (2, BANDS, NX, NZ, NY), 1.0, 6.0, ((1, 16), (2, 32)), jnp.float32),
        "potential": jnp.clip(jax.random.uniform(keys[2], (NX, NZ, NY), jnp.float32, -1.5, 1.5) * shard_levels(keys[2], (NX, NZ, NY), ((0, 16), (1, 32)), -0.4, 0.0), -1.5, 1.5),
        "column_extent": draw_column_extent(jax.random.fold_in(keys[7], 71), 0),
        "metric": jnp.clip(jnp.exp(jax.random.uniform(keys[4], (3,), jnp.float32, math.log(0.5), math.log(2.0))), 0.5, 2.0),
        "center": jnp.clip(jax.random.uniform(keys[5], (1,), jnp.float32, 0.5, 2.0), 0.5, 2.0),
        "halfwidth": jnp.clip(jnp.exp(jax.random.uniform(keys[6], (1,), jnp.float32, math.log(1.0), math.log(3.0))), 1.0, 3.0),
    }


def signed(length):
    indices = jnp.arange(length, dtype=jnp.int32)
    return jnp.where(indices < length // 2, indices, indices - length)


def reference(wave, previous, potential, column_extent, metric, center, halfwidth):
    keep_mask = (jnp.abs(signed(NZ))[None, :, None] <= column_extent[:, None, :]).astype(jnp.float32)
    two_pi = 2.0 * math.pi
    kinetic_x = (two_pi * signed(NX).astype(jnp.float32) / NX) ** 2
    kinetic_y = (two_pi * signed(NY).astype(jnp.float32) / NY) ** 2
    kinetic_z = (two_pi * signed(NZ).astype(jnp.float32) / NZ) ** 2
    kinetic = 0.5 * (metric[0] * kinetic_x[:, None, None] + metric[2] * kinetic_z[None, :, None] + metric[1] * kinetic_y[None, None, :])
    cell_count = NX * NY * NZ
    factor = 2.0 / halfwidth[0]

    def one_band(pieces):
        real_in, imag_in, real_prev, imag_prev = pieces
        coefficient = (real_in + 1j * imag_in) * keep_mask
        real_space = jnp.fft.ifftn(coefficient) * cell_count
        potential_term = jnp.fft.fftn(potential * real_space) / cell_count
        applied = kinetic * coefficient + potential_term
        result = keep_mask * (factor * (applied - center[0] * coefficient) - (real_prev + 1j * imag_prev))
        return jnp.real(result).astype(jnp.float32), jnp.imag(result).astype(jnp.float32)

    real_out, imag_out = lax.map(one_band, (wave[0], wave[1], previous[0], previous[1]))
    return jnp.stack([real_out, imag_out])
```

```python
import math

import jax
import jax.numpy as jnp
import numpy as np
from jax import lax
from jax.experimental import pallas as pl
from jax.experimental.pallas import tpu as pltpu
from jax.sharding import PartitionSpec as P

N = 128
H = 32
K = 2 * H
F32 = jnp.float32
BF16 = jnp.bfloat16


def kept():
    g = np.arange(K)
    return np.where(g < H, g, g + N - K)


def angles(rows, cols):
    return 2.0 * math.pi * ((rows[:, None] * cols[None, :]) % N) / N


def lanes():
    g = np.concatenate([np.arange(H), np.arange(N - H, N), np.arange(H), np.arange(N - H, N)])
    imag = np.repeat([0, 1, 1, 0], H)
    return g, imag


def split_table(table):
    hi = table.astype(np.float32).astype(BF16)
    lo = (table - hi.astype(np.float64)).astype(np.float32).astype(BF16)
    return hi, lo


def z_inverse_table():
    theta = angles(np.arange(N), kept())
    both = np.concatenate([np.cos(theta), np.sin(theta)], axis=1)
    out = np.zeros((N // 4, 2, 4, 2, 2 * K))
    for b in range(2):
        out[:, b, :, b, :] = both.reshape(N // 4, 4, 2 * K)
    return out.reshape(2 * N, 4 * K)


def z_forward_table():
    theta = angles(kept(), np.arange(N))
    out = np.zeros((2, 2, K, N // 4, 2, 4))
    for b in range(2):
        out[0, b, :, :, b, :] = np.cos(theta).reshape(K, N // 4, 4) / N
        out[1, b, :, :, b, :] = np.sin(theta).reshape(K, N // 4, 4) / N
    return out.reshape(4 * K, 2 * N)


def y_inverse_table():
    g, imag = lanes()
    theta = angles(g, np.arange(N))
    re = np.where(imag[:, None] == 0, np.cos(theta), -np.sin(theta))
    im = np.where(imag[:, None] == 0, np.sin(theta), np.cos(theta))
    return np.concatenate([re, im], axis=1)


def y_forward_table():
    g, imag = lanes()
    theta = angles(np.arange(N), g)
    re = np.where(imag[None, :] == 0, np.cos(theta), -np.sin(theta))
    im = np.where(imag[None, :] == 0, np.sin(theta), np.cos(theta))
    return np.concatenate([re, im], axis=0) / N


def x_inverse_table():
    theta = angles(np.arange(N), kept())
    c, s = np.cos(theta), np.sin(theta)
    return np.block([[c, -s], [s, c]])


def x_forward_table():
    theta = angles(kept(), np.arange(N))
    c, s = np.cos(theta), np.sin(theta)
    return np.block([[c, s], [-s, c]]) / N


def split(value):
    hi = value.astype(BF16)
    return hi, (value - hi.astype(F32)).astype(BF16)


def mm(a, b):
    return jnp.dot(a, b, preferred_element_type=F32)


def outer_lanes(shape):
    lane = lax.broadcasted_iota(jnp.int32, shape, 1)
    return (lane < H) | (lane >= N - H)


def kept_abs(shape):
    row = lax.broadcasted_iota(jnp.int32, shape, 0)
    return jnp.where(row < H, row, K - row)


def kept_rows(ref, *index):
    return jnp.concatenate([ref[(*index, slice(0, H))], ref[(*index, slice(N - H, N))]], axis=0)


def z_inverse_kernel(wave_ref, extent_ref, th_ref, tl_ref, o_ref):
    outer = outer_lanes((K, N))
    sign = jnp.where(outer, -1.0, 1.0)
    size = kept_abs((K, N))
    for gx in range(4):
        keep = size <= extent_ref[gx : gx + 1, :]
        rows = []
        for b in range(2):
            re = jnp.where(keep, kept_rows(wave_ref, 0, b, gx), 0.0)
            im = jnp.where(keep, kept_rows(wave_ref, 1, b, gx), 0.0)
            x = jnp.where(outer, re, pltpu.roll(im, N // 2, 1))
            rows += [x, pltpu.roll(x, N // 2, 1) * sign]
        hi, lo = split(jnp.concatenate(rows, axis=0))
        out = mm(th_ref[...], hi) + mm(th_ref[...], lo) + mm(tl_ref[...], hi)
        o_ref[:, 8 * gx : 8 * gx + 8, :] = out.reshape(N // 4, 8, N)


def middle_kernel(
    r_ref, v_ref, yi_ref, yil_ref, xi_ref, xil_ref, xf_ref, xfl_ref, yf_ref, yfl_ref, o_ref
):
    band = lax.axis_index("band")
    my_x, my_z = band // 4, band % 4
    v = []
    for z in range(4):
        parts = []
        for j in range(16):
            slot = ((my_x - j // 4 + 4) % 4) * 4 + (my_z - j % 4 + 4) % 4
            parts.append(v_ref[pl.ds(slot * 32 + z, 8, stride=4), :])
        v.append(jnp.concatenate(parts, axis=0))
    for z in range(4):
        rows = []
        for p in (z, 4 + z):
            rows += [r_ref[pl.ds(p, H, stride=8), :], r_ref[pl.ds(8 * (N - H) + p, H, stride=8), :]]
        hi, lo = split(jnp.concatenate(rows, axis=0))
        y = mm(hi, yi_ref[...]) + mm(lo, yi_ref[...]) + mm(hi, yil_ref[...])
        f = jnp.concatenate(
            [
                jnp.concatenate([y[:K, :N], y[:K, N:]], axis=0),
                jnp.concatenate([y[K:, :N], y[K:, N:]], axis=0),
            ],
            axis=1,
        )
        hi, lo = split(f)
        s = mm(xi_ref[...], hi) + mm(xi_ref[...], lo) + mm(xil_ref[...], hi)
        vz = jnp.concatenate([v[z], v[z]], axis=0)
        s = s * jnp.concatenate([vz, vz], axis=1)
        hi, lo = split(s)
        g = mm(xf_ref[...], hi) + mm(xf_ref[...], lo) + mm(xfl_ref[...], hi)
        rows = jnp.concatenate(
            [
                jnp.concatenate([g[:K, :N], g[K:, :N]], axis=1),
                jnp.concatenate([g[:K, N:], g[K:, N:]], axis=1),
            ],
            axis=0,
        )
        hi, lo = split(rows)
        out = mm(hi, yf_ref[...]) + mm(lo, yf_ref[...]) + mm(hi, yfl_ref[...])
        for b in range(2):
            p = 4 * b + z
            o_ref[pl.ds(p, H, stride=8), :] = out[b * K : b * K + H]
            o_ref[pl.ds(8 * (N - H) + p, H, stride=8), :] = out[b * K + H : b * K + K]
    o_ref[8 * H : 8 * (N - H), :] = jnp.zeros((8 * (N - K), N), F32)


def update_kernel(
    r_ref, wave_ref, previous_ref, extent_ref, zh_ref, zl_ref, metric_ref, center_ref, half_ref, o_ref
):
    outer = outer_lanes((K, N))
    sign = jnp.where(outer, -1.0, 1.0)
    size = kept_abs((K, N))
    two_pi = 2.0 * math.pi
    lane = lax.broadcasted_iota(jnp.int32, (K, N), 1)
    signed_y = jnp.where(lane < N // 2, lane, lane - N)
    kinetic_y = (two_pi * signed_y.astype(F32) / N) ** 2
    kinetic_z = (two_pi * size.astype(F32) / N) ** 2
    factor = 2.0 / half_ref[0]
    center = center_ref[0]
    zeros = jnp.zeros((N - K, N), F32)
    for gx in range(4):
        hi, lo = split(r_ref[:, 8 * gx : 8 * gx + 8, :].reshape(2 * N, N))
        pq = mm(zh_ref[...], hi) + mm(zh_ref[...], lo) + mm(zl_ref[...], hi)
        keep = size <= extent_ref[gx : gx + 1, :]
        index_x = jnp.full((K, N), lax.axis_index("fft") * 4 + gx, jnp.int32)
        signed_x = jnp.where(index_x < N // 2, index_x, index_x - N)
        kinetic_x = (two_pi * signed_x.astype(F32) / N) ** 2
        kinetic = 0.5 * (
            metric_ref[0] * kinetic_x + metric_ref[2] * kinetic_z + metric_ref[1] * kinetic_y
        )
        for b in range(2):
            p, q = pq[b * K : b * K + K], pq[2 * K + b * K : 2 * K + b * K + K]
            applied = p - pltpu.roll(q, N // 2, 1) * sign
            for part, term in ((0, applied), (1, pltpu.roll(applied, N // 2, 1))):
                c = kept_rows(wave_ref, part, b, gx)
                value = factor * (kinetic * c + term - center * c) - kept_rows(
                    previous_ref, part, b, gx
                )
                value = jnp.where(keep, value, 0.0)
                o_ref[part, b, gx, 0:H, :] = value[:H]
                o_ref[part, b, gx, H : N - H, :] = zeros
                o_ref[part, b, gx, N - H : N, :] = value[H:]


VMEM = pl.BlockSpec(memory_space=pltpu.VMEM)
SMEM = pl.BlockSpec(memory_space=pltpu.SMEM)


def call(kernel, shape, specs, name, flops):
    return pl.pallas_call(
        kernel,
        out_shape=jax.ShapeDtypeStruct(shape, F32),
        in_specs=specs,
        out_specs=VMEM,
        name=name,
        cost_estimate=pl.CostEstimate(flops=flops, bytes_accessed=2 << 20, transcendentals=0),
        compiler_params=pltpu.CompilerParams(vmem_limit_bytes=16 << 20),
    )


def swap(blocks):
    return lax.all_to_all(blocks, "fft", split_axis=0, concat_axis=0, tiled=True)


def gather_potential(potential):
    own = potential.reshape(32, N)
    band = range(16)

    def shift(value, dx, dz):
        pairs = [(i, (i // 4 + dx) % 4 * 4 + (i % 4 + dz) % 4) for i in band]
        return lax.ppermute(value, "band", pairs)

    line = jnp.concatenate([own] + [shift(own, 0, s) for s in (1, 2, 3)], axis=0)
    return jnp.concatenate([line] + [shift(line, t, 0) for t in (1, 2, 3)], axis=0)


def local(wave, previous, potential, column_extent, metric, center, halfwidth):
    zi, zf = split_table(z_inverse_table()), split_table(z_forward_table())
    yi, yf = split_table(y_inverse_table()), split_table(y_forward_table())
    xi, xf = split_table(x_inverse_table()), split_table(x_forward_table())
    v = gather_potential(potential)
    blocks = call(z_inverse_kernel, (32, 32, N), [VMEM] * 4, "z_inverse", 200_000_000)(
        wave, column_extent, *zi
    )
    blocks = swap(blocks).reshape(1024, N)
    blocks = call(middle_kernel, (1024, N), [VMEM] * 10, "middle", 800_000_000)(
        blocks, v, *yi, *xi, *xf, *yf
    )
    blocks = swap(blocks.reshape(32, 32, N))
    return call(update_kernel, wave.shape, [VMEM] * 6 + [SMEM] * 3, "update", 200_000_000)(
        blocks, wave, previous, column_extent, *zf, metric, center, halfwidth
    )


def solution(mesh):
    in_specs = (
        P(None, "band", "fft", None, None),
        P(None, "band", "fft", None, None),
        P("band", "fft", None),
        P("fft", None),
        P(),
        P(),
        P(),
    )
    out_specs = P(None, "band", "fft", None, None)
    return jax.shard_map(local, mesh=mesh, in_specs=in_specs, out_specs=out_specs, check_vma=False)
```

```python
import math

import jax
import jax.numpy as jnp
import numpy as np
from jax import lax
from jax.experimental import pallas as pl
from jax.experimental.pallas import tpu as pltpu
from jax.sharding import PartitionSpec as P

N = 128
H = 32
K = 2 * H
F32 = jnp.float32
BF16 = jnp.bfloat16


def kept():
    g = np.arange(K)
    return np.where(g < H, g, g + N - K)


def angles(rows, cols):
    return 2.0 * math.pi * ((rows[:, None] * cols[None, :]) % N) / N


def lanes():
    g = np.concatenate([np.arange(H), np.arange(N - H, N), np.arange(H), np.arange(N - H, N)])
    imag = np.repeat([0, 1, 1, 0], H)
    return g, imag


def split_table(table):
    hi = table.astype(np.float32).astype(BF16)
    lo = (table - hi.astype(np.float64)).astype(np.float32).astype(BF16)
    return hi, lo


def z_inverse_table():
    theta = angles(np.arange(N), kept())
    both = np.concatenate([np.cos(theta), np.sin(theta)], axis=1)
    out = np.zeros((N // 4, 2, 4, 2, 2 * K))
    for b in range(2):
        out[:, b, :, b, :] = both.reshape(N // 4, 4, 2 * K)
    return out.reshape(2 * N, 4 * K)


def z_forward_table():
    theta = angles(kept(), np.arange(N))
    out = np.zeros((2, 2, K, N // 4, 2, 4))
    for b in range(2):
        out[0, b, :, :, b, :] = np.cos(theta).reshape(K, N // 4, 4) / N
        out[1, b, :, :, b, :] = np.sin(theta).reshape(K, N // 4, 4) / N
    return out.reshape(4 * K, 2 * N)


def y_inverse_table():
    g, imag = lanes()
    theta = angles(g, np.arange(N))
    re = np.where(imag[:, None] == 0, np.cos(theta), -np.sin(theta))
    im = np.where(imag[:, None] == 0, np.sin(theta), np.cos(theta))
    return np.concatenate([re, im], axis=1)


def y_forward_table():
    g, imag = lanes()
    theta = angles(np.arange(N), g)
    re = np.where(imag[None, :] == 0, np.cos(theta), -np.sin(theta))
    im = np.where(imag[None, :] == 0, np.sin(theta), np.cos(theta))
    return np.concatenate([re, im], axis=0) / N


def x_inverse_table():
    theta = angles(np.arange(N), kept())
    c, s = np.cos(theta), np.sin(theta)
    return np.block([[c, -s], [s, c]])


def x_forward_table():
    theta = angles(kept(), np.arange(N))
    c, s = np.cos(theta), np.sin(theta)
    return np.block([[c, s], [-s, c]]) / N


def split(value):
    hi = value.astype(BF16)
    return hi, (value - hi.astype(F32)).astype(BF16)


def mm(a, b):
    return jnp.dot(a, b, preferred_element_type=F32)


def outer_lanes(shape):
    lane = lax.broadcasted_iota(jnp.int32, shape, 1)
    return (lane < H) | (lane >= N - H)


def kept_abs(shape):
    row = lax.broadcasted_iota(jnp.int32, shape, 0)
    return jnp.where(row < H, row, K - row)


def kept_rows(ref, *index):
    return jnp.concatenate([ref[(*index, slice(0, H))], ref[(*index, slice(N - H, N))]], axis=0)


def z_inverse_kernel(
    wave_hbm, extent_hbm, th_hbm, tl_hbm, o_ref, wave_ref, extent_ref, th_ref, tl_ref, sems
):
    copies = [
        pltpu.make_async_copy(extent_hbm, extent_ref, sems.at[0]),
        pltpu.make_async_copy(
            wave_hbm.at[:, :, :, 0:H, :], wave_ref.at[:, :, :, 0:H, :], sems.at[1]
        ),
        pltpu.make_async_copy(
            wave_hbm.at[:, :, :, N - H : N, :], wave_ref.at[:, :, :, H:K, :], sems.at[2]
        ),
        pltpu.make_async_copy(th_hbm, th_ref, sems.at[3]),
        pltpu.make_async_copy(tl_hbm, tl_ref, sems.at[4]),
    ]
    for copy in copies:
        copy.start()
    outer = outer_lanes((K, N))
    sign = jnp.where(outer, -1.0, 1.0)
    size = kept_abs((K, N))
    for copy in copies:
        copy.wait()
    for gx in range(4):
        keep = size <= extent_ref[gx : gx + 1, :]
        rows = []
        for b in range(2):
            re = jnp.where(keep, wave_ref[0, b, gx], 0.0)
            im = jnp.where(keep, wave_ref[1, b, gx], 0.0)
            x = jnp.where(outer, re, pltpu.roll(im, N // 2, 1))
            rows += [x, pltpu.roll(x, N // 2, 1) * sign]
        hi, lo = split(jnp.concatenate(rows, axis=0))
        out = mm(th_ref[...], hi) + mm(th_ref[...], lo) + mm(tl_ref[...], hi)
        o_ref[:, 8 * gx : 8 * gx + 8, :] = out.reshape(N // 4, 8, N)


def middle_kernel(
    r_ref, near_ref, far_ref, yi_ref, yil_ref, xi_ref, xil_ref, xf_ref, xfl_ref, yf_ref, yfl_ref, o_ref
):
    band = lax.axis_index("band")
    my_x, my_z = band // 4, band % 4
    v = []
    for z in range(4):
        parts = []
        for j in range(16):
            dx, dz = my_x ^ (j // 4), my_z ^ (j % 4)
            slot = (dx ^ (dx // 2)) * 4 + (dz ^ (dz // 2))
            start = (slot % 8) * 32 + z
            parts.append(
                jnp.where(
                    slot < 8,
                    near_ref[pl.ds(start, 8, stride=4), :],
                    far_ref[pl.ds(start, 8, stride=4), :],
                )
            )
        v.append(jnp.concatenate(parts, axis=0))
    for z in range(4):
        rows = []
        for p in (z, 4 + z):
            rows += [r_ref[pl.ds(p, H, stride=8), :], r_ref[pl.ds(8 * (N - H) + p, H, stride=8), :]]
        hi, lo = split(jnp.concatenate(rows, axis=0))
        y = mm(hi, yi_ref[...]) + mm(lo, yi_ref[...]) + mm(hi, yil_ref[...])
        f = jnp.concatenate(
            [
                jnp.concatenate([y[:K, :N], y[:K, N:]], axis=0),
                jnp.concatenate([y[K:, :N], y[K:, N:]], axis=0),
            ],
            axis=1,
        )
        hi, lo = split(f)
        s = mm(xi_ref[...], hi) + mm(xi_ref[...], lo) + mm(xil_ref[...], hi)
        vz = jnp.concatenate([v[z], v[z]], axis=0)
        s = s * jnp.concatenate([vz, vz], axis=1)
        hi, lo = split(s)
        g = mm(xf_ref[...], hi) + mm(xf_ref[...], lo) + mm(xfl_ref[...], hi)
        rows = jnp.concatenate(
            [
                jnp.concatenate([g[:K, :N], g[K:, :N]], axis=1),
                jnp.concatenate([g[:K, N:], g[K:, N:]], axis=1),
            ],
            axis=0,
        )
        hi, lo = split(rows)
        out = mm(hi, yf_ref[...]) + mm(lo, yf_ref[...]) + mm(hi, yfl_ref[...])
        for b in range(2):
            p = 4 * b + z
            o_ref[pl.ds(p, H, stride=8), :] = out[b * K : b * K + H]
            o_ref[pl.ds(8 * (N - H) + p, H, stride=8), :] = out[b * K + H : b * K + K]
    o_ref[8 * H : 8 * (N - H), :] = jnp.zeros((8 * (N - K), N), F32)


def update_kernel(
    r_ref, wave_ref, previous_ref, extent_ref, zh_ref, zl_ref, metric_ref, center_ref, half_ref, o_ref
):
    outer = outer_lanes((K, N))
    sign = jnp.where(outer, -1.0, 1.0)
    size = kept_abs((K, N))
    two_pi = 2.0 * math.pi
    lane = lax.broadcasted_iota(jnp.int32, (K, N), 1)
    signed_y = jnp.where(lane < N // 2, lane, lane - N)
    kinetic_y = (two_pi * signed_y.astype(F32) / N) ** 2
    kinetic_z = (two_pi * size.astype(F32) / N) ** 2
    factor = 2.0 / half_ref[0]
    center = center_ref[0]
    zeros = jnp.zeros((N - K, N), F32)
    for gx in range(4):
        hi, lo = split(r_ref[:, 8 * gx : 8 * gx + 8, :].reshape(2 * N, N))
        pq = mm(zh_ref[...], hi) + mm(zh_ref[...], lo) + mm(zl_ref[...], hi)
        keep = size <= extent_ref[gx : gx + 1, :]
        index_x = jnp.full((K, N), lax.axis_index("fft") * 4 + gx, jnp.int32)
        signed_x = jnp.where(index_x < N // 2, index_x, index_x - N)
        kinetic_x = (two_pi * signed_x.astype(F32) / N) ** 2
        kinetic = 0.5 * (
            metric_ref[0] * kinetic_x + metric_ref[2] * kinetic_z + metric_ref[1] * kinetic_y
        )
        for b in range(2):
            p, q = pq[b * K : b * K + K], pq[2 * K + b * K : 2 * K + b * K + K]
            applied = p - pltpu.roll(q, N // 2, 1) * sign
            for part, term in ((0, applied), (1, pltpu.roll(applied, N // 2, 1))):
                c = kept_rows(wave_ref, part, b, gx)
                value = factor * (kinetic * c + term - center * c) - kept_rows(
                    previous_ref, part, b, gx
                )
                value = jnp.where(keep, value, 0.0)
                o_ref[part, b, gx, 0:H, :] = value[:H]
                o_ref[part, b, gx, H : N - H, :] = zeros
                o_ref[part, b, gx, N - H : N, :] = value[H:]


VMEM = pl.BlockSpec(memory_space=pltpu.VMEM)
SMEM = pl.BlockSpec(memory_space=pltpu.SMEM)
HBM = pl.BlockSpec(memory_space=pltpu.HBM)


def call(kernel, shape, specs, flops, scratch=()):
    return pl.pallas_call(
        kernel,
        out_shape=jax.ShapeDtypeStruct(shape, F32),
        in_specs=specs,
        out_specs=VMEM,
        scratch_shapes=list(scratch),
        cost_estimate=pl.CostEstimate(flops=flops, bytes_accessed=2 << 20, transcendentals=0),
        compiler_params=pltpu.CompilerParams(vmem_limit_bytes=16 << 20),
    )


def swap(blocks):
    return lax.all_to_all(blocks, "fft", split_axis=0, concat_axis=0, tiled=True)


def exchange(value, dx, dz):
    pairs = [(i, (i // 4 ^ dx) * 4 + (i % 4 ^ dz)) for i in range(16)]
    return lax.ppermute(value, "band", pairs)


def gather_potential(potential):
    near = potential.reshape(32, N)
    for dx, dz in ((0, 1), (0, 3), (1, 0)):
        near = jnp.concatenate([near, exchange(near, dx, dz)], axis=0)
    return near, exchange(near, 3, 0)


def local(wave, previous, potential, column_extent, metric, center, halfwidth):
    zi, zf = split_table(z_inverse_table()), split_table(z_forward_table())
    yi, yf = split_table(y_inverse_table()), split_table(y_forward_table())
    xi, xf = split_table(x_inverse_table()), split_table(x_forward_table())
    near, far = gather_potential(potential)
    scratch = [
        pltpu.VMEM((2, 2, 4, K, N), F32),
        pltpu.VMEM((4, N), jnp.int32),
        pltpu.VMEM((2 * N, 4 * K), BF16),
        pltpu.VMEM((2 * N, 4 * K), BF16),
        pltpu.SemaphoreType.DMA((5,)),
    ]
    blocks = call(z_inverse_kernel, (32, 32, N), [HBM] * 4, 200_000_000, scratch)(
        wave, column_extent, *zi
    )
    blocks = swap(blocks).reshape(1024, N)
    blocks = call(middle_kernel, (1024, N), [VMEM] * 11, 800_000_000)(
        blocks, near, far, *yi, *xi, *xf, *yf
    )
    blocks = swap(blocks.reshape(32, 32, N))
    return call(update_kernel, wave.shape, [VMEM] * 6 + [SMEM] * 3, 200_000_000)(
        blocks, wave, previous, column_extent, *zf, metric, center, halfwidth
    )


def solution(mesh):
    in_specs = (
        P(None, "band", "fft", None, None),
        P(None, "band", "fft", None, None),
        P("band", "fft", None),
        P("fft", None),
        P(),
        P(),
        P(),
    )
    out_specs = P(None, "band", "fft", None, None)
    return jax.shard_map(local, mesh=mesh, in_specs=in_specs, out_specs=out_specs, check_vma=False)
```

```python
import math

import jax
import jax.numpy as jnp
import numpy as np
from jax import lax
from jax.experimental import pallas as pl
from jax.experimental.pallas import tpu as pltpu
from jax.sharding import PartitionSpec as P

N = 128
H = 32
K = 2 * H
F32 = jnp.float32
BF16 = jnp.bfloat16


def kept():
    g = np.arange(K)
    return np.where(g < H, g, g + N - K)


def angles(rows, cols):
    return 2.0 * math.pi * ((rows[:, None] * cols[None, :]) % N) / N


def lanes():
    g = np.concatenate([np.arange(H), np.arange(N - H, N), np.arange(H), np.arange(N - H, N)])
    imag = np.repeat([0, 1, 1, 0], H)
    return g, imag


def split_table(table):
    hi = table.astype(np.float32).astype(BF16)
    lo = (table - hi.astype(np.float64)).astype(np.float32).astype(BF16)
    return hi, lo


def z_inverse_table():
    theta = angles(np.arange(N), kept())
    both = np.concatenate([np.cos(theta), np.sin(theta)], axis=1)
    out = np.zeros((N // 4, 2, 4, 2, 2 * K))
    for b in range(2):
        out[:, b, :, b, :] = both.reshape(N // 4, 4, 2 * K)
    return out.reshape(2 * N, 4 * K)


def z_forward_table():
    theta = angles(kept(), np.arange(N))
    out = np.zeros((2, 2, K, N // 4, 2, 4))
    for b in range(2):
        out[0, b, :, :, b, :] = np.cos(theta).reshape(K, N // 4, 4) / N
        out[1, b, :, :, b, :] = np.sin(theta).reshape(K, N // 4, 4) / N
    return out.reshape(4 * K, 2 * N)


def y_inverse_table():
    g, imag = lanes()
    theta = angles(g, np.arange(N))
    re = np.where(imag[:, None] == 0, np.cos(theta), -np.sin(theta))
    im = np.where(imag[:, None] == 0, np.sin(theta), np.cos(theta))
    return np.concatenate([re, im], axis=1)


def y_forward_table():
    g, imag = lanes()
    theta = angles(np.arange(N), g)
    re = np.where(imag[None, :] == 0, np.cos(theta), -np.sin(theta))
    im = np.where(imag[None, :] == 0, np.sin(theta), np.cos(theta))
    return np.concatenate([re, im], axis=0) / N


def x_inverse_table():
    theta = angles(np.arange(N), kept())
    c, s = np.cos(theta), np.sin(theta)
    return np.block([[c, -s], [s, c]])


def x_forward_table():
    theta = angles(kept(), np.arange(N))
    c, s = np.cos(theta), np.sin(theta)
    return np.block([[c, s], [-s, c]]) / N


def split(value):
    hi = value.astype(BF16)
    return hi, (value - hi.astype(F32)).astype(BF16)


def mm(a, b):
    return jnp.dot(a, b, preferred_element_type=F32)


def outer_lanes(shape):
    lane = lax.broadcasted_iota(jnp.int32, shape, 1)
    return (lane < H) | (lane >= N - H)


def kept_abs(shape):
    row = lax.broadcasted_iota(jnp.int32, shape, 0)
    return jnp.where(row < H, row, K - row)


def kept_rows(ref, *index):
    return jnp.concatenate([ref[(*index, slice(0, H))], ref[(*index, slice(N - H, N))]], axis=0)


def z_inverse_kernel(
    wave_hbm, extent_hbm, th_hbm, tl_hbm, o_ref, wave_ref, extent_ref, th_ref, tl_ref, sems
):
    copies = [
        pltpu.make_async_copy(extent_hbm, extent_ref, sems.at[0]),
        pltpu.make_async_copy(
            wave_hbm.at[:, :, :, 0:H, :], wave_ref.at[:, :, :, 0:H, :], sems.at[1]
        ),
        pltpu.make_async_copy(
            wave_hbm.at[:, :, :, N - H : N, :], wave_ref.at[:, :, :, H:K, :], sems.at[2]
        ),
        pltpu.make_async_copy(th_hbm, th_ref, sems.at[3]),
        pltpu.make_async_copy(tl_hbm, tl_ref, sems.at[4]),
    ]
    for copy in copies:
        copy.start()
    outer = outer_lanes((K, N))
    sign = jnp.where(outer, -1.0, 1.0)
    size = kept_abs((K, N))
    for copy in copies:
        copy.wait()
    for gx in range(4):
        keep = size <= extent_ref[gx : gx + 1, :]
        rows = []
        for b in range(2):
            re = jnp.where(keep, wave_ref[0, b, gx], 0.0)
            im = jnp.where(keep, wave_ref[1, b, gx], 0.0)
            x = jnp.where(outer, re, pltpu.roll(im, N // 2, 1))
            rows += [x, pltpu.roll(x, N // 2, 1) * sign]
        hi, lo = split(jnp.concatenate(rows, axis=0))
        out = mm(th_ref[...], hi) + mm(th_ref[...], lo) + mm(tl_ref[...], hi)
        o_ref[:, 8 * gx : 8 * gx + 8, :] = out.reshape(N // 4, 8, N)


def inverse_kernel(
    r_ref,
    yi_ref,
    yil_ref,
    xi_ref,
    xil_ref,
    extent_ref,
    metric_ref,
    center_ref,
    half_ref,
    s_ref,
    aux_ref,
):
    aux_ref[0:4, :] = extent_ref[...].astype(F32)
    row = lax.broadcasted_iota(jnp.int32, (4, N), 0)
    metric = jnp.where(row == 1, metric_ref[0], jnp.where(row == 2, metric_ref[1], metric_ref[2]))
    aux_ref[4:8, :] = jnp.where(row == 0, center_ref[0], metric)
    aux_ref[8:16, :] = jnp.full((8, N), 2.0 / half_ref[0], F32)
    for z in range(4):
        rows = []
        for p in (z, 4 + z):
            rows += [r_ref[pl.ds(p, H, stride=8), :], r_ref[pl.ds(8 * (N - H) + p, H, stride=8), :]]
        hi, lo = split(jnp.concatenate(rows, axis=0))
        y = mm(jnp.concatenate([hi, lo], axis=1), yi_ref[...]) + mm(hi, yil_ref[...])
        f = jnp.concatenate(
            [
                jnp.concatenate([y[:K, :N], y[:K, N:]], axis=0),
                jnp.concatenate([y[K:, :N], y[K:, N:]], axis=0),
            ],
            axis=1,
        )
        hi, lo = split(f)
        s = mm(xi_ref[...], jnp.concatenate([hi, lo], axis=0)) + mm(xil_ref[...], hi)
        s_ref[:, 2 * N * z : 2 * N * (z + 1)] = s


def forward_kernel(
    s_ref, v0_ref, v1_ref, v3_ref, v2_ref, xf_ref, xfl_ref, yf_ref, o_ref, v_ref
):
    band = lax.axis_index("band")
    my_x, my_z = band // 4, band % 4
    for dz, ref in ((0, v0_ref), (1, v1_ref), (3, v3_ref), (2, v2_ref)):
        v_ref[pl.ds(pl.multiple_of((my_z ^ dz) * N, N), N), :] = ref[...]
    for z in range(4):
        parts = []
        for j in range(16):
            dx = my_x ^ (j // 4)
            slot = 4 * (j % 4) + (dx ^ (dx // 2))
            parts.append(v_ref[pl.ds(slot * 32 + z, 8, stride=4), :])
        v = jnp.concatenate(parts, axis=0)
        v = jnp.concatenate([v, v], axis=0)
        s = s_ref[:, 2 * N * z : 2 * N * (z + 1)] * jnp.concatenate([v, v], axis=1)
        hi, lo = split(s)
        g = mm(xf_ref[...], hi) + mm(xf_ref[...], lo) + mm(xfl_ref[...], hi)
        rows = jnp.concatenate(
            [
                jnp.concatenate([g[:K, :N], g[K:, :N]], axis=1),
                jnp.concatenate([g[:K, N:], g[K:, N:]], axis=1),
            ],
            axis=0,
        )
        hi, lo = split(rows)
        both = mm(hi, yf_ref[...])
        out = both[:, :N] + both[:, N:] + mm(lo, yf_ref[:, :N])
        for b in range(2):
            p = 4 * b + z
            o_ref[pl.ds(p, H, stride=8), :] = out[b * K : b * K + H]
            o_ref[pl.ds(8 * (N - H) + p, H, stride=8), :] = out[b * K + H : b * K + K]
    o_ref[8 * H : 8 * (N - H), :] = jnp.zeros((8 * (N - K), N), F32)


def update_kernel(r_ref, wave_ref, previous_ref, aux_ref, zh_ref, zl_ref, o_ref):
    outer = outer_lanes((K, N))
    sign = jnp.where(outer, -1.0, 1.0)
    size = kept_abs((K, N)).astype(F32)
    two_pi = 2.0 * math.pi
    lane = lax.broadcasted_iota(jnp.int32, (K, N), 1)
    signed_y = jnp.where(lane < N // 2, lane, lane - N)
    kinetic_y = (two_pi * signed_y.astype(F32) / N) ** 2
    kinetic_z = (two_pi * size / N) ** 2
    kinetic_zy = aux_ref[7:8, :] * kinetic_z + aux_ref[6:7, :] * kinetic_y
    center, factor = aux_ref[4:5, :], aux_ref[8:9, :]
    zeros = jnp.zeros((N - K, N), F32)
    for gx in range(4):
        hi, lo = split(r_ref[:, 8 * gx : 8 * gx + 8, :].reshape(2 * N, N))
        pq = mm(zh_ref[...], hi) + mm(zh_ref[...], lo) + mm(zl_ref[...], hi)
        keep = size <= aux_ref[gx : gx + 1, :]
        index_x = jnp.full((K, N), lax.axis_index("fft") * 4 + gx, jnp.int32)
        signed_x = jnp.where(index_x < N // 2, index_x, index_x - N)
        kinetic_x = (two_pi * signed_x.astype(F32) / N) ** 2
        scale = 0.5 * (aux_ref[5:6, :] * kinetic_x + kinetic_zy) - center
        for b in range(2):
            p, q = pq[b * K : b * K + K], pq[2 * K + b * K : 2 * K + b * K + K]
            applied = p - pltpu.roll(q, N // 2, 1) * sign
            for part, term in ((0, applied), (1, pltpu.roll(applied, N // 2, 1))):
                value = factor * (scale * kept_rows(wave_ref, part, b, gx) + term)
                value = jnp.where(keep, value - kept_rows(previous_ref, part, b, gx), 0.0)
                o_ref[part, b, gx, 0:H, :] = value[:H]
                o_ref[part, b, gx, H : N - H, :] = zeros
                o_ref[part, b, gx, N - H : N, :] = value[H:]


VMEM = pl.BlockSpec(memory_space=pltpu.VMEM)
SMEM = pl.BlockSpec(memory_space=pltpu.SMEM)
HBM = pl.BlockSpec(memory_space=pltpu.HBM)


def call(kernel, shape, specs, flops, scratch=(), limit=16 << 20):
    return pl.pallas_call(
        kernel,
        out_shape=[jax.ShapeDtypeStruct(one, F32) for one in shape],
        in_specs=specs,
        out_specs=[VMEM] * len(shape),
        scratch_shapes=list(scratch),
        cost_estimate=pl.CostEstimate(flops=flops, bytes_accessed=2 << 20, transcendentals=0),
        compiler_params=pltpu.CompilerParams(vmem_limit_bytes=limit),
    )


def swap(blocks):
    return lax.all_to_all(blocks, "fft", split_axis=0, concat_axis=0, tiled=True)


def exchange(value, dx, dz):
    pairs = [(i, (i // 4 ^ dx) * 4 + (i % 4 ^ dz)) for i in range(16)]
    return lax.ppermute(value, "band", pairs)


def gather_potential(potential):
    line = potential.reshape(32, N)
    for dx in (1, 3):
        line = jnp.concatenate([line, exchange(line, dx, 0)], axis=0)
    return [line] + [exchange(line, 0, dz) for dz in (1, 3, 2)]


def local(wave, previous, potential, column_extent, metric, center, halfwidth):
    zi, zf = split_table(z_inverse_table()), split_table(z_forward_table())
    yi, yf = split_table(y_inverse_table()), split_table(y_forward_table())
    xi, xf = split_table(x_inverse_table()), split_table(x_forward_table())
    scratch = [
        pltpu.VMEM((2, 2, 4, K, N), F32),
        pltpu.VMEM((4, N), jnp.int32),
        pltpu.VMEM((2 * N, 4 * K), BF16),
        pltpu.VMEM((2 * N, 4 * K), BF16),
        pltpu.SemaphoreType.DMA((5,)),
    ]
    (blocks,) = call(z_inverse_kernel, [(32, 32, N)], [HBM] * 4, 200_000_000, scratch, 63 << 20)(
        wave, column_extent, *zi
    )
    pieces = gather_potential(potential)
    blocks = swap(blocks).reshape(1024, N)
    shapes = [(2 * N, 8 * N), (16, N)]
    field, aux = call(inverse_kernel, shapes, [VMEM] * 6 + [SMEM] * 3, 400_000_000)(
        blocks,
        np.concatenate([yi[0], yi[0]], axis=0),
        yi[1],
        np.concatenate([xi[0], xi[0]], axis=1),
        xi[1],
        column_extent,
        metric,
        center,
        halfwidth,
    )
    scratch = [pltpu.VMEM((4 * N, N), F32)]
    (blocks,) = call(
        forward_kernel, [(1024, N)], [VMEM] * 8, 400_000_000, scratch
    )(field, *pieces, *xf, np.concatenate(yf, axis=1))
    blocks = swap(blocks.reshape(32, 32, N))
    (out,) = call(update_kernel, [wave.shape], [VMEM] * 6, 200_000_000)(
        blocks, wave, previous, aux, *zf
    )
    return out


def solution(mesh):
    in_specs = (
        P(None, "band", "fft", None, None),
        P(None, "band", "fft", None, None),
        P("band", "fft", None),
        P("fft", None),
        P(),
        P(),
        P(),
    )
    out_specs = P(None, "band", "fft", None, None)
    return jax.shard_map(local, mesh=mesh, in_specs=in_specs, out_specs=out_specs, check_vma=False)
```
